32 devices in a mesh: days: 4 (over y, x), space: 8 (over z, core).
Axes of the slice: x: 2, y: 2, z: 4, core: 2. Of those that a mesh axis runs over, the one named last changes fastest.
Arguments:
- fields: bfloat16 [640, 32, 1440], P('days', 'space')
- month_label: int32 [640], P('days'), may hold values from 0 to 11, as said below
- row_index: int32 [32], P('space'), may hold values from 0 to 31
- area_table: float32 [32], replicated, may hold values from 0.05 to 1
- basis: bfloat16 [64, 32, 1440], P(None, 'space'), may hold values from -6 to 6
Outputs:
- eofs: float32 [64, 32, 1440], P(None, 'space')
- pcs: float32 [640, 64], P('days')
The draws below stay inside these ranges and needn't reach their ends.
Inputs may be any that keep to these rules, and one draw needn't show every extreme that they name: `month_label`: each day's label differs from floor(12 * day / 640) by at most one; the first day with a given value of floor(12 * day / 640) carries exactly that value; every month labels at least one day.
All inputs are finite; a program needn't handle non-finite values.
Results may differ from the reference program's by a relative error of at most 0.0003.
Values sent between devices are 32-bit elements; how exact they have to be, the bound alone decides.
A program may use at most 64 MiB of HBM per device.

```python
import math
import jax
import jax.numpy as jnp
from jax import lax

LON = 1440
MODES = 64
ITERS = 2
LAT_DEV = 4
LAT = 32
DAYS = 640
N_SPACE = 8


def month_series(key):
    day = jnp.arange(DAYS, dtype=jnp.int32)
    base = day * 12 // DAYS
    first = base != (day - 1) * 12 // DAYS
    jitter = jax.random.randint(jax.random.fold_in(key, 7), (DAYS,), -1, 2)
    return jnp.where(first, base, jnp.clip(base + jitter, 0, 11)).astype(jnp.int32)


def draw_month_label(key, part):
    return month_series(key)


def draw_fields(key, part):
    labels = month_series(key)
    season = jax.random.normal(jax.random.fold_in(key, 11), (12, LAT, LON), jnp.float32)
    noise = jax.random.normal(jax.random.fold_in(key, 13), (DAYS, LAT, LON), jnp.float32)
    values = 2.0 * season[labels] + noise
    return values.astype(jnp.bfloat16)


def touch_ends(entries, rng, low, top_value):
    dims = entries.shape
    place = [jax.random.randint(jax.random.fold_in(rng, axis), (), 0, dims[axis]) for axis in range(len(dims))]
    entries = entries.at[tuple(place)].set(low)
    longest = dims.index(max(dims))
    place[longest] = (place[longest] + 1) % dims[longest]
    return entries.at[tuple(place)].set(top_value)


def block_scale(rng, extent, shards, smallest, top_value):
    gain, own = 1.0, jax.random.fold_in(rng, 6)
    for dim, shards_of in shards:
        steps = jnp.exp(jax.random.uniform(jax.random.fold_in(own, dim), (shards_of,), jnp.float32, smallest / len(shards), top_value / len(shards)))
        gain = gain * jnp.repeat(steps, extent[dim] // shards_of).reshape([-1 if axis == dim else 1 for axis in range(len(extent))])
    return gain


def scatter_about(own_key, dims, deviation, bound, cuts=(), kind=jnp.bfloat16):
    values = jax.random.normal(own_key, dims, jnp.float32) * deviation
    if len(cuts) > 0:
        values = block_scale(own_key, dims, cuts, -0.22, 0.18) * values
    return jnp.clip(values, min=-bound, max=bound).astype(kind)


def setup_inputs(seed: int = 0) -> dict:
    seeds = jax.random.split(jax.random.key(seed), 6)
    fields = draw_fields(jax.random.fold_in(seeds[5], 71), 0)
    month_label = draw_month_label(jax.random.fold_in(seeds[5], 71), 0)
    row_index = touch_ends(jax.random.randint(seeds[2], (LAT,), 0, LAT), jax.random.fold_in(seeds[2], 1), 0, LAT - 1).astype(jnp.int32)
    area_table = jnp.clip(jnp.exp(jax.random.uniform(seeds[3], (LAT,), jnp.float32, math.log(0.05), math.log(1.0))), 0.05, 1.0)
    basis = scatter_about(seeds[4], (MODES, LAT, LON), 1.0, 6.0, ((1, 8),))
    return dict(fields=fields, month_label=month_label, row_index=row_index, area_table=area_table, basis=basis)


HIGH = lax.Precision.HIGHEST

def reference(fields, month_label, row_index, area_table, basis):
    months = jnp.arange(12, dtype=jnp.int32)
    onehot = (month_label[None, :] == months[:, None]).astype(jnp.float32)
    counts = lax.optimization_barrier(jnp.sum(onehot, axis=1))

    def block_fields(index):
        return lax.dynamic_slice_in_dim(fields, (index * LAT_DEV).astype(jnp.int32), LAT_DEV, 1).astype(jnp.float32)

    def add_sums(index):
        return jnp.einsum('md,dlc->mlc', onehot, block_fields(index), precision=HIGH)
    sums = lax.map(add_sums, jnp.arange(N_SPACE, dtype=jnp.int32))
    climate = sums / counts[None, :, None, None]
    scale = jnp.sqrt(area_table[row_index])

    def anomaly(index):
        seasonal = jnp.einsum('md,mlc->dlc', onehot, climate[index], precision=HIGH)
        rows = lax.dynamic_slice_in_dim(scale, (index * LAT_DEV).astype(jnp.int32), LAT_DEV, 0)
        return (block_fields(index) - seasonal) * rows[None, :, None]

    def project(patterns):

        def step(total, index):
            piece = lax.dynamic_slice_in_dim(patterns, (index * LAT_DEV).astype(jnp.int32), LAT_DEV, 1)
            return (total + jnp.einsum('dlc,klc->dk', anomaly(index), piece, precision=HIGH), None)
        start = jnp.zeros((DAYS, MODES), jnp.float32)
        total, _ = lax.scan(step, start, jnp.arange(N_SPACE, dtype=jnp.int32))
        return total
    pcs = project(basis.astype(jnp.float32))
    for step_count in range(ITERS):

        def cover_block(index):
            return jnp.einsum('dk,dlc->klc', pcs, anomaly(index), precision=HIGH) / DAYS
        blocks = lax.map(cover_block, jnp.arange(N_SPACE, dtype=jnp.int32))
        cover = jnp.moveaxis(blocks, 0, 1).reshape(MODES, LAT * LON)
        gram = jnp.dot(cover, cover.T, precision=HIGH)
        lower = jnp.linalg.cholesky(gram)
        solved = lax.linalg.triangular_solve(lower, cover, left_side=True, lower=True)
        eofs = solved.reshape(MODES, LAT, LON)
        pcs = project(eofs)
    return (eofs, pcs)
```

```python
import functools

import jax
import jax.numpy as jnp
from jax import lax
from jax.experimental import pallas as pl
from jax.experimental.pallas import tpu as pltpu
from jax.sharding import PartitionSpec as P

ITERS = 2
MESH = pl.DeviceIdType.MESH
HIGH = lax.Precision.HIGHEST
F32 = jnp.float32
BF16 = jnp.bfloat16
LANES = 128


def up(value, step):
    return -(-value // step) * step


def nt(a, b, **kw):
    return lax.dot_general(a, b, (((1,), (1,)), ((), ())), preferred_element_type=F32, **kw)


def nn(a, b, **kw):
    return lax.dot_general(a, b, (((1,), (0,)), ((), ())), preferred_element_type=F32, **kw)


def split3(x):
    high = x.astype(BF16)
    rest = x - high.astype(F32)
    mid = rest.astype(BF16)
    low = (rest - mid.astype(F32)).astype(BF16)
    return jnp.concatenate([high, mid, low], axis=0)


def join3(x, n):
    return x[:n] + (x[n : 2 * n] + x[2 * n :])


def inverse_factor(gram):
    n = gram.shape[0]
    sub = lax.broadcasted_iota(jnp.int32, (n, 1), 0)
    eye = (lax.broadcasted_iota(jnp.int32, (n, n), 0) == lax.broadcasted_iota(jnp.int32, (n, n), 1)).astype(F32)
    work = jnp.concatenate([gram, eye], axis=1)
    for j in range(n):
        row = work[j : j + 1, :]
        column = work[:, j : j + 1]
        inv = lax.rsqrt(work[j : j + 1, j : j + 1])
        row = row * inv
        work = jnp.where(sub == j, row, work - jnp.where(sub > j, column * inv, 0.0) * row)
    return work[:, n:]


def kernel(nd, ns, days_total, f_ref, b_ref, s_ref, e_ref, eofs_ref, pcs_ref,
           send_f, recv_f, full_f, p_part, p_rs, p_mine, p_all, q_all,
           x_out, x_rs, x_day, x_all, c_all, tall,
           sem_f, sem_prs, sem_pag, sem_pd, sem_xrs, sem_xd, sem_xag, sem_c):
    lat, dl, lon = f_ref.shape
    modes = eofs_ref.shape[1]
    rows = lat // nd
    day, space = lax.axis_index("days"), lax.axis_index("space")

    def peer(me, k, n):
        return lax.rem(me + k, n), lax.rem(me + n - k, n)

    def copy(src, dst, sems, index, axis, target):
        return pltpu.make_async_remote_copy(
            src_ref=src, dst_ref=dst, send_sem=sems.at[(0,) + index], recv_sem=sems.at[(1,) + index],
            device_id={axis: target}, device_id_type=MESH)

    barrier = pltpu.get_barrier_semaphore()
    for k in range(1, nd):
        pl.semaphore_signal(barrier, inc=1, device_id={"days": peer(day, k, nd)[0]}, device_id_type=MESH)
    for k in range(1, ns):
        pl.semaphore_signal(barrier, inc=1, device_id={"space": peer(space, k, ns)[0]}, device_id_type=MESH)
    pl.semaphore_wait(barrier, nd + ns - 2)

    f_sent = []
    for k in range(1, nd):
        to = peer(day, k, nd)[0]
        for r in range(rows):
            send_f[k - 1, r] = f_ref[to * rows + r].astype(F32)
        c = copy(send_f.at[k - 1], recv_f.at[day], sem_f, (k - 1,), "days", to)
        c.start()
        f_sent.append(c)

    total = None
    for l in range(lat):
        term = nt(f_ref[l], b_ref[l]) * s_ref[l]
        total = term if total is None else total + term
    height = p_part.shape[1]
    p_part[...] = jnp.zeros_like(p_part)
    for t in range(ns):
        have = min(dl, (t + 1) * height) - t * height
        if have > 0:
            p_part[t, :have] = total[t * height : t * height + have]
    sent = []
    for k in range(1, ns):
        to = peer(space, k, ns)[0]
        c = copy(p_part.at[to], p_rs.at[k - 1], sem_prs, (k - 1,), "space", to)
        c.start()
        sent.append(c)
    acc = p_part[space]
    for k in range(1, ns):
        sent[k - 1].wait()
        acc = acc + p_rs[k - 1]
    p_all[space] = acc
    sent = []
    for k in range(1, ns):
        to = peer(space, k, ns)[0]
        c = copy(p_all.at[space], p_all.at[space], sem_pag, (k - 1,), "space", to)
        c.start()
        sent.append(c)
    for k in range(1, ns):
        sent[k - 1].wait_send()
        frm = peer(space, k, ns)[1]
        copy(p_all.at[frm], p_all.at[frm], sem_pag, (k - 1,), "space", frm).wait_recv()
    p_mine[...] = jnp.concatenate([p_all[t] for t in range(ns)], axis=0)[:dl] + e_ref[...]
    sent = []
    q_all[day] = p_mine[...]
    for k in range(1, nd):
        to = peer(day, k, nd)[0]
        c = copy(p_mine, q_all.at[day], sem_pd, (k - 1,), "days", to)
        c.start()
        sent.append(c)
    for r in range(rows):
        full_f[r, pl.ds(pl.multiple_of(day * dl, 16), dl)] = f_ref[day * rows + r]
    for k in range(1, nd):
        sent[k - 1].wait_send()
        frm = peer(day, k, nd)[1]
        copy(p_mine, q_all.at[frm], sem_pd, (k - 1,), "days", frm).wait_recv()
    qt = jnp.concatenate([q_all[j] for j in range(nd)], axis=0).T
    start = qt[:modes]
    months = qt[LANES // 2 :] if modes <= LANES // 2 else qt[up(modes, LANES) :]
    mean_of = months / jnp.maximum(jnp.sum(months, axis=1, keepdims=True), 1.0)

    def center(x):
        return x - nn(nt(x, mean_of, precision=HIGH), months, precision=HIGH)

    pcs = center(start)
    for k in range(1, nd):
        f_sent[k - 1].wait_send()
        frm = peer(day, k, nd)[1]
        copy(send_f.at[k - 1], recv_f.at[frm], sem_f, (k - 1,), "days", frm).wait_recv()
        for r in range(rows):
            full_f[r, pl.ds(pl.multiple_of(frm * dl, 16), dl)] = recv_f[frm, r].astype(BF16)

    part = modes // ns
    n_days = nd * dl
    gram_at = up(n_days, LANES)
    for it in range(ITERS):
        last = it == ITERS - 1
        pcs3 = split3(pcs)
        gram, raw = None, None
        for r in range(rows):
            scale = s_ref[day * rows + r]
            cover = join3(nn(pcs3, full_f[r]), modes) * (scale * (1.0 / days_total))
            if last:
                c_all[day, r] = cover
            term = nt(cover, cover, precision=HIGH)
            gram = term if gram is None else gram + term
            term = join3(nt(split3(cover * scale), full_f[r]), modes)
            raw = term if raw is None else raw + term
        x_out[it, :, :n_days] = raw
        x_out[it, :, n_days:] = jnp.zeros((modes, x_out.shape[2] - n_days), F32)
        x_out[it, :, gram_at : gram_at + modes] = gram
        sent = []
        for k in range(1, ns):
            to = peer(space, k, ns)[0]
            c = copy(x_out.at[it, pl.ds(pl.multiple_of(to * part, part), part)], x_rs.at[it, k - 1],
                     sem_xrs, (it, k - 1), "space", to)
            c.start()
            sent.append(c)
        acc = x_out[it, pl.ds(pl.multiple_of(space * part, part), part)]
        for k in range(1, ns):
            sent[k - 1].wait()
            acc = acc + x_rs[it, k - 1]
        x_day[it, day] = acc
        sent = []
        for k in range(1, nd):
            to = peer(day, k, nd)[0]
            c = copy(x_day.at[it, day], x_day.at[it, day], sem_xd, (it, k - 1), "days", to)
            c.start()
            sent.append(c)
        c_sent = []
        if last:
            for k in range(1, nd):
                to = peer(day, k, nd)[0]
                c = copy(c_all.at[day], c_all.at[day], sem_c, (k - 1,), "days", to)
                c.start()
                c_sent.append(c)
        for k in range(1, nd):
            sent[k - 1].wait_send()
            frm = peer(day, k, nd)[1]
            copy(x_day.at[it, frm], x_day.at[it, frm], sem_xd, (it, k - 1), "days", frm).wait_recv()
        acc = x_day[it, 0]
        for j in range(1, nd):
            acc = acc + x_day[it, j]
        x_all[it, space] = acc
        sent = []
        for k in range(1, ns):
            to = peer(space, k, ns)[0]
            c = copy(x_all.at[it, space], x_all.at[it, space], sem_xag, (it, k - 1), "space", to)
            c.start()
            sent.append(c)
        for k in range(1, ns):
            sent[k - 1].wait_send()
            frm = peer(space, k, ns)[1]
            copy(x_all.at[it, frm], x_all.at[it, frm], sem_xag, (it, k - 1), "space", frm).wait_recv()
        whole = jnp.concatenate([x_all[it, t] for t in range(ns)], axis=0)
        inv = inverse_factor(whole[:, gram_at : gram_at + modes])
        raw = center(whole[:, :n_days])
        if not last:
            pcs = nn(inv, raw, precision=HIGH)
    tall[...] = raw.T
    mine = tall[pl.ds(pl.multiple_of(day * dl, 8), dl)]
    pcs_ref[...] = nt(mine, inv, precision=HIGH)
    for r in range(rows):
        eofs_ref[day * rows + r] = nn(inv, c_all[day, r], precision=HIGH)
    for k in range(1, nd):
        c_sent[k - 1].wait_send()
        frm = peer(day, k, nd)[1]
        copy(c_all.at[frm], c_all.at[frm], sem_c, (k - 1,), "days", frm).wait_recv()
        for r in range(rows):
            eofs_ref[frm * rows + r] = nn(inv, c_all[frm, r], precision=HIGH)


def solution(mesh):
    nd, ns = mesh.shape["days"], mesh.shape["space"]

    def local(fields, month_label, row_index, area_table, basis):
        dl, lat, lon = fields.shape
        modes = basis.shape[0]
        rows = lat // nd
        part = modes // ns
        group = up(modes, LANES // 2)
        wide = up(group + 12, LANES)
        height = up(-(-dl // ns), 8)
        n_days = nd * dl
        span = up(n_days, LANES) + up(modes, LANES)
        table_hot = (row_index[:, None] == jnp.arange(area_table.shape[0], dtype=jnp.int32)[None, :]).astype(F32)
        scale = jnp.sqrt(jnp.sum(table_hot * area_table[None, :], axis=1))
        extra = (month_label[:, None] == jnp.arange(wide, dtype=jnp.int32)[None, :] - group).astype(F32)
        f_t = jnp.transpose(fields, (1, 0, 2))
        b_t = jnp.pad(jnp.transpose(basis, (1, 0, 2)), ((0, 0), (0, wide - modes), (0, 0)))
        v, dma = pltpu.VMEM, pltpu.SemaphoreType.DMA
        eofs, pcs = pl.pallas_call(
            functools.partial(kernel, nd, ns, n_days),
            out_shape=(jax.ShapeDtypeStruct((lat, modes, lon), F32), jax.ShapeDtypeStruct((dl, modes), F32)),
            in_specs=[pl.BlockSpec(memory_space=v)] * 4,
            out_specs=(pl.BlockSpec(memory_space=v),) * 2,
            scratch_shapes=[
                v((nd - 1, rows, dl, lon), F32),
                v((nd, rows, dl, lon), F32),
                v((rows, n_days, lon), BF16),
                v((ns, height, wide), F32),
                v((ns - 1, height, wide), F32),
                v((dl, wide), F32),
                v((ns, height, wide), F32),
                v((nd, dl, wide), F32),
                v((ITERS, modes, span), F32),
                v((ITERS, ns - 1, part, span), F32),
                v((ITERS, nd, part, span), F32),
                v((ITERS, ns, part, span), F32),
                v((nd, rows, modes, lon), F32),
                v((n_days, modes), F32),
                dma((2, nd - 1)), dma((2, ns - 1)), dma((2, ns - 1)), dma((2, nd - 1)),
                dma((2, ITERS, ns - 1)), dma((2, ITERS, nd - 1)), dma((2, ITERS, ns - 1)), dma((2, nd - 1)),
            ],
            compiler_params=pltpu.CompilerParams(
                collective_id=0, has_side_effects=True, vmem_limit_bytes=60 * 1024 * 1024),
        )(f_t, b_t, jnp.broadcast_to(scale[:, None, None], (lat, 1, LANES))[:, :, :1], extra)
        return jnp.transpose(eofs, (1, 0, 2)), pcs

    placed = (P("days", "space", None), P("days"), P("space"), P(), P(None, "space", None))
    return jax.shard_map(
        local,
        mesh=mesh,
        in_specs=placed,
        out_specs=(P(None, "space", None), P("days", None)),
        check_vma=False,
    )
```

```python
import functools

import jax
import jax.numpy as jnp
from jax import lax
from jax.experimental import pallas as pl
from jax.experimental.pallas import tpu as pltpu
from jax.sharding import PartitionSpec as P

ITERS = 2
MESH = pl.DeviceIdType.MESH
HIGH = lax.Precision.HIGHEST
F32 = jnp.float32
BF16 = jnp.bfloat16
LANES = 128


def up(value, step):
    return -(-value // step) * step


def nt(a, b, **kw):
    return lax.dot_general(a, b, (((1,), (1,)), ((), ())), preferred_element_type=F32, **kw)


def nn(a, b, **kw):
    return lax.dot_general(a, b, (((1,), (0,)), ((), ())), preferred_element_type=F32, **kw)


def split3(x):
    high = x.astype(BF16)
    rest = x - high.astype(F32)
    mid = rest.astype(BF16)
    low = (rest - mid.astype(F32)).astype(BF16)
    return jnp.concatenate([high, mid, low], axis=0)


def join3(x, n):
    return x[:n] + (x[n : 2 * n] + x[2 * n :])


def inverse_factor(gram):
    n = gram.shape[0]
    sub = lax.broadcasted_iota(jnp.int32, (n, 1), 0)
    eye = (lax.broadcasted_iota(jnp.int32, (n, n), 0) == lax.broadcasted_iota(jnp.int32, (n, n), 1)).astype(F32)
    work = jnp.concatenate([gram, eye], axis=1)
    for j in range(n):
        row = work[j : j + 1, :]
        column = work[:, j : j + 1]
        inv = lax.rsqrt(work[j : j + 1, j : j + 1])
        row = row * inv
        work = jnp.where(sub == j, row, work - jnp.where(sub > j, column * inv, 0.0) * row)
    return work[:, n:]


def kernel(nd, ns, days_total, f_ref, b_ref, i_ref, a_ref, l_ref, eofs_ref, pcs_ref,
           send_f, recv_f, full_f, p_part, p_rs, p_mine, p_all, q_all,
           x_out, x_rs, x_day, x_all, c_all, tall, s_ref,
           sem_f, sem_prs, sem_pag, sem_pd, sem_xrs, sem_xd, sem_xag, sem_c):
    lat, dl, lon = f_ref.shape
    modes = eofs_ref.shape[0]
    rows = lat // nd
    day, space = lax.axis_index("days"), lax.axis_index("space")

    def peer(me, k, n):
        if n & (n - 1):
            return lax.rem(me + k, n), lax.rem(me + n - k, n)
        other = me
        for bit in range(n.bit_length()):
            if (k >> bit) & 1:
                other = other + (1 << bit) * (1 - 2 * lax.rem(lax.div(me, 1 << bit), 2))
        return other, other

    def copy(src, dst, sems, index, axis, target):
        return pltpu.make_async_remote_copy(
            src_ref=src, dst_ref=dst, send_sem=sems.at[(0,) + index], recv_sem=sems.at[(1,) + index],
            device_id={axis: target}, device_id_type=MESH)

    barrier = pltpu.get_barrier_semaphore()
    for k in range(1, nd):
        pl.semaphore_signal(barrier, inc=1, device_id={"days": peer(day, k, nd)[0]}, device_id_type=MESH)
    for k in range(1, ns):
        pl.semaphore_signal(barrier, inc=1, device_id={"space": peer(space, k, ns)[0]}, device_id_type=MESH)
    pl.semaphore_wait(barrier, nd + ns - 2)

    f_sent = []

    def send_fields(k):
        to = peer(day, k, nd)[0]
        for r in range(rows):
            send_f[k - 1, r] = f_ref[to * rows + r].astype(F32)
        c = copy(send_f.at[k - 1], recv_f.at[day], sem_f, (k - 1,), "days", to)
        c.start()
        f_sent.append(c)

    for k in range(1, nd - 1):
        send_fields(k)
    scales = [jnp.sqrt(jnp.full((1, 1), a_ref[i_ref[l]], F32)) for l in range(lat)]
    for l in range(lat):
        s_ref[l] = scales[l]

    total = None
    for l in range(lat):
        term = nt(f_ref[l], b_ref[:, l, :]) * scales[l]
        total = term if total is None else total + term
    height, wide = p_part.shape[1:]
    total = jnp.concatenate([total, jnp.zeros((dl, wide - modes), F32)], axis=1)
    p_part[...] = jnp.zeros_like(p_part)
    for t in range(ns):
        have = min(dl, (t + 1) * height) - t * height
        if have > 0:
            p_part[t, :have] = total[t * height : t * height + have]
    sent = []
    for k in range(1, ns):
        to = peer(space, k, ns)[0]
        c = copy(p_part.at[to], p_rs.at[k - 1], sem_prs, (k - 1,), "space", to)
        c.start()
        sent.append(c)
    acc = p_part[space]
    for k in range(1, ns):
        sent[k - 1].wait()
        acc = acc + p_rs[k - 1]
    p_all[space] = acc
    sent = []
    for k in range(1, ns):
        to = peer(space, k, ns)[0]
        c = copy(p_all.at[space], p_all.at[space], sem_pag, (k - 1,), "space", to)
        c.start()
        sent.append(c)
    for k in range(1, ns):
        sent[k - 1].wait_send()
        frm = peer(space, k, ns)[1]
        copy(p_all.at[frm], p_all.at[frm], sem_pag, (k - 1,), "space", frm).wait_recv()
    group = up(modes, LANES // 2)
    hot = (l_ref[...] == lax.broadcasted_iota(jnp.int32, (wide, dl), 0) - group).astype(F32)
    p_mine[...] = jnp.concatenate([p_all[t] for t in range(ns)], axis=0)[:dl] + hot.T
    sent = []
    q_all[day] = p_mine[...]
    for k in range(1, nd):
        to = peer(day, k, nd)[0]
        c = copy(p_mine, q_all.at[day], sem_pd, (k - 1,), "days", to)
        c.start()
        sent.append(c)
    send_fields(nd - 1)
    for r in range(rows):
        full_f[r, pl.ds(pl.multiple_of(day * dl, 16), dl)] = f_ref[day * rows + r]
    for k in range(1, nd):
        sent[k - 1].wait_send()
        frm = peer(day, k, nd)[1]
        copy(p_mine, q_all.at[frm], sem_pd, (k - 1,), "days", frm).wait_recv()
    qt = jnp.concatenate([q_all[j] for j in range(nd)], axis=0).T
    start = qt[:modes]
    months = qt[LANES // 2 :] if modes <= LANES // 2 else qt[up(modes, LANES) :]
    mean_of = months / jnp.maximum(jnp.sum(months, axis=1, keepdims=True), 1.0)

    def center(x):
        return x - nn(nt(x, mean_of, precision=HIGH), months, precision=HIGH)

    pcs = center(start)
    for k in range(1, nd):
        f_sent[k - 1].wait_send()
        frm = peer(day, k, nd)[1]
        copy(send_f.at[k - 1], recv_f.at[frm], sem_f, (k - 1,), "days", frm).wait_recv()
        for r in range(rows):
            full_f[r, pl.ds(pl.multiple_of(frm * dl, 16), dl)] = recv_f[frm, r].astype(BF16)

    part = modes // ns
    n_days = nd * dl
    gram_at = up(n_days, LANES)
    for it in range(ITERS):
        last = it == ITERS - 1
        pcs3 = split3(pcs)
        gram, raw = None, None
        for r in range(rows):
            scale = s_ref[day * rows + r]
            cover = join3(nn(pcs3, full_f[r]), modes) * (scale * (1.0 / days_total))
            if last:
                c_all[day, r] = cover
            term = nt(cover, cover, precision=HIGH)
            gram = term if gram is None else gram + term
            term = join3(nt(split3(cover * scale), full_f[r]), modes)
            raw = term if raw is None else raw + term
        x_out[it, :, :n_days] = raw
        x_out[it, :, n_days:] = jnp.zeros((modes, x_out.shape[2] - n_days), F32)
        x_out[it, :, gram_at : gram_at + modes] = gram
        sent = []
        for k in range(1, ns):
            to = peer(space, k, ns)[0]
            c = copy(x_out.at[it, pl.ds(pl.multiple_of(to * part, part), part)], x_rs.at[it, k - 1],
                     sem_xrs, (it, k - 1), "space", to)
            c.start()
            sent.append(c)
        acc = x_out[it, pl.ds(pl.multiple_of(space * part, part), part)]
        for k in range(1, ns):
            sent[k - 1].wait()
            acc = acc + x_rs[it, k - 1]
        x_day[it, day] = acc
        sent = []
        for k in range(1, nd):
            to = peer(day, k, nd)[0]
            c = copy(x_day.at[it, day], x_day.at[it, day], sem_xd, (it, k - 1), "days", to)
            c.start()
            sent.append(c)
        c_sent = []
        if last:
            for k in range(1, nd):
                to = peer(day, k, nd)[0]
                c = copy(c_all.at[day], c_all.at[day], sem_c, (k - 1,), "days", to)
                c.start()
                c_sent.append(c)
        for k in range(1, nd):
            sent[k - 1].wait_send()
            frm = peer(day, k, nd)[1]
            copy(x_day.at[it, frm], x_day.at[it, frm], sem_xd, (it, k - 1), "days", frm).wait_recv()
        acc = x_day[it, 0]
        for j in range(1, nd):
            acc = acc + x_day[it, j]
        x_all[it, space] = acc
        sent = []
        for k in range(1, ns):
            to = peer(space, k, ns)[0]
            c = copy(x_all.at[it, space], x_all.at[it, space], sem_xag, (it, k - 1), "space", to)
            c.start()
            sent.append(c)
        for k in range(1, ns):
            sent[k - 1].wait_send()
            frm = peer(space, k, ns)[1]
            copy(x_all.at[it, frm], x_all.at[it, frm], sem_xag, (it, k - 1), "space", frm).wait_recv()
        whole = jnp.concatenate([x_all[it, t] for t in range(ns)], axis=0)
        inv = inverse_factor(whole[:, gram_at : gram_at + modes])
        raw = center(whole[:, :n_days])
        if not last:
            pcs = nn(inv, raw, precision=HIGH)
    tall[...] = raw.T
    mine = tall[pl.ds(pl.multiple_of(day * dl, 8), dl)]
    pcs_ref[...] = nt(inv, mine, precision=HIGH)
    for k in range(1, nd):
        c_sent[k - 1].wait_send()
        frm = peer(day, k, nd)[1]
        copy(c_all.at[frm], c_all.at[frm], sem_c, (k - 1,), "days", frm).wait_recv()
    for j in range(nd):
        for r in range(rows):
            eofs_ref[:, j * rows + r, :] = nn(inv, c_all[j, r], precision=HIGH)


def solution(mesh):
    nd, ns = mesh.shape["days"], mesh.shape["space"]

    def local(fields, month_label, row_index, area_table, basis):
        dl, lat, lon = fields.shape
        modes = basis.shape[0]
        rows = lat // nd
        part = modes // ns
        group = up(modes, LANES // 2)
        wide = up(group + 12, LANES)
        height = up(-(-dl // ns), 8)
        n_days = nd * dl
        span = up(n_days, LANES) + up(modes, LANES)
        f_t = jnp.transpose(fields, (1, 0, 2))
        v, dma = pltpu.VMEM, pltpu.SemaphoreType.DMA
        eofs, pcs = pl.pallas_call(
            functools.partial(kernel, nd, ns, n_days),
            out_shape=(jax.ShapeDtypeStruct((modes, lat, lon), F32), jax.ShapeDtypeStruct((modes, dl), F32)),
            in_specs=[pl.BlockSpec(memory_space=v)] * 2 + [pl.BlockSpec(memory_space=pltpu.SMEM)] * 2
            + [pl.BlockSpec(memory_space=v)],
            out_specs=(pl.BlockSpec(memory_space=v),) * 2,
            scratch_shapes=[
                v((nd - 1, rows, dl, lon), F32),
                v((nd, rows, dl, lon), F32),
                v((rows, n_days, lon), BF16),
                v((ns, height, wide), F32),
                v((ns - 1, height, wide), F32),
                v((dl, wide), F32),
                v((ns, height, wide), F32),
                v((nd, dl, wide), F32),
                v((ITERS, modes, span), F32),
                v((ITERS, ns - 1, part, span), F32),
                v((ITERS, nd, part, span), F32),
                v((ITERS, ns, part, span), F32),
                v((nd, rows, modes, lon), F32),
                v((n_days, modes), F32),
                v((lat, 1, 1), F32),
                dma((2, nd - 1)), dma((2, ns - 1)), dma((2, ns - 1)), dma((2, nd - 1)),
                dma((2, ITERS, ns - 1)), dma((2, ITERS, nd - 1)), dma((2, ITERS, ns - 1)), dma((2, nd - 1)),
            ],
            compiler_params=pltpu.CompilerParams(
                collective_id=0, has_side_effects=True, vmem_limit_bytes=60 * 1024 * 1024),
        )(f_t, basis, row_index, area_table, month_label[None, :])
        return eofs, pcs.T

    placed = (P("days", "space", None), P("days"), P("space"), P(), P(None, "space", None))
    return jax.shard_map(
        local,
        mesh=mesh,
        in_specs=placed,
        out_specs=(P(None, "space", None), P("days", None)),
        check_vma=False,
    )
```
